128 devices in a mesh: grp: 8 (over x, core), shard: 16 (over z, y).
Axes of the slice: x: 4, y: 4, z: 4, core: 2. Of those that a mesh axis runs over, the one named last changes fastest.
Arguments:
- activations: bfloat16 [1, 24576, 5120], P(None, ('grp', 'shard')), may hold values from -6 to 6
- out_grads: bfloat16 [1, 24576, 5120], P(None, ('grp', 'shard')), may hold values from -0.107910156 to 0.107910156
- error: float32 [8, 5120, 1, 5120], P('grp', 'shard'), may hold values from -6 to 6
- q_start: float32 [1, 32, 5120], replicated, may hold values from -6 to 6
Outputs:
- update: float32 [5120, 1, 5120], P('shard')
- error_next: float32 [8, 5120, 1, 5120], P('grp', 'shard')
- factor: float32 [1, 32, 5120], replicated
The draws below stay inside these ranges and needn't reach their ends.
All inputs are finite; a program needn't handle non-finite values.
Results may differ from the reference program's by a relative error of at most 0.0034.
Values may be sent and summed in bfloat16 or wider, within the bound.
No kernel may reach another device: no remote copies, remote signals or barrier semaphores. Data moves between devices by JAX's collectives and lax.ppermute only.
A program may use at most 256 MiB of HBM per device.

```python
import jax
import jax.numpy as jnp
from jax import lax

DW = 5120
RANK = 32
MATS = 1
ITERS = 2
TOK_DEV = 192
GROUPS = 8
GROUP_TOK = 3072
TOKENS = 24576
N_SHARD = 16


def levels(own_key, extent, shards, low, largest):
    gain, own = 1.0, jax.random.fold_in(own_key, 6)
    for axis_at, blocks in shards:
        heights = jnp.exp(jax.random.uniform(jax.random.fold_in(own, axis_at), (blocks,), jnp.float32, low / len(shards), largest / len(shards)))
        gain = gain * jnp.repeat(heights, extent[axis_at] // blocks).reshape([-1 if axis == axis_at else 1 for axis in range(len(extent))])
    return gain


def bell_draw(key, extent, scale, limit, cuts=(), dtype=jnp.bfloat16):
    values = jax.random.normal(key, extent, jnp.float32) * scale
    if len(cuts) > 0:
        values = levels(key, extent, cuts, -0.22, 0.18) * values
    return jnp.clip(values, min=-limit, max=limit).astype(dtype)


def setup_inputs(seed: int = 0) -> dict:
    seeds = jax.random.split(jax.random.key(seed), 5)
    return {
        "activations": bell_draw(seeds[0], (MATS, TOKENS, DW), 1.0, 6.0, ((1, 128),)),
        "out_grads": bell_draw(seeds[1], (MATS, TOKENS, DW), (GROUP_TOK ** -0.5), 0.107910156, ((1, 128),)),
        "error": bell_draw(seeds[2], (GROUPS, DW, MATS, DW), 1.0, 6.0, ((0, 8), (1, 16)), jnp.float32),
        "q_start": bell_draw(seeds[3], (MATS, RANK, DW), 1.0, 6.0, (), jnp.float32),
    }


def group_gradient(pair):
    inputs, grads = pair

    def accumulate(running, piece):
        left_in, right_in = piece
        partial_sum = jnp.einsum('mta,mtc->amc', left_in.astype(jnp.float32), right_in.astype(jnp.float32))
        rounded = lax.optimization_barrier(partial_sum.astype(jnp.bfloat16)).astype(jnp.float32)
        return (running + rounded, None)
    start_sum = jnp.zeros((DW, MATS, DW), jnp.float32)
    running, unused = lax.scan(accumulate, start_sum, (inputs, grads))
    return running

def reference(activations, out_grads, error, q_start):
    shaped_in = activations.reshape(MATS, GROUPS, N_SHARD, TOK_DEV, DW).transpose(1, 2, 0, 3, 4)
    shaped_grad = out_grads.reshape(MATS, GROUPS, N_SHARD, TOK_DEV, DW).transpose(1, 2, 0, 3, 4)
    gradient = lax.map(group_gradient, (shaped_in, shaped_grad))
    momentum = gradient + error
    right = q_start
    high = lax.Precision.HIGHEST
    for step in range(ITERS):
        left = jnp.einsum('grmc,mkc->rmk', momentum, right, precision=high) / GROUPS
        gram = jnp.einsum('rmk,rml->mkl', left, left, precision=high)
        lower = jnp.linalg.cholesky(gram)
        basis = jax.vmap(lambda tri, rhs: jax.scipy.linalg.solve_triangular(tri, rhs, lower=True))(lower, left.transpose(1, 2, 0))
        right = jnp.einsum('mkr,grmc->mkc', basis, momentum, precision=high) / GROUPS
    update = jnp.einsum('mkr,mkc->rmc', basis, right, precision=high)
    return (update, momentum - update[None], right)
```

```python
import functools

import jax
import jax.numpy as jnp
from jax import lax
from jax.experimental import pallas as pl
from jax.experimental.pallas import tpu as pltpu
from jax.sharding import Mesh
from jax.sharding import PartitionSpec as P

GRP = ("x", "c")
SHARD = ("z", "y")
ALL = ("x", "c", "z", "y")
BF = jnp.bfloat16
F32 = jnp.float32
HIGH = lax.Precision.HIGHEST
ITERS = 2
LANES = 128
HEIGHT = 256


def shift(v, axis, by):
    n = lax.axis_size(axis)
    return lax.ppermute(v, axis, [(i, (i + by) % n) for i in range(n)])


def swapped(v):
    n = lax.axis_size("x")
    pairs = [(i * n + j, j * n + i) for i in range(n) for j in range(n)]
    return lax.ppermute(v, ("x", "y"), pairs)


def times(a, b, dims):
    return lax.dot_general(a, b, (dims, ((), ())), precision=HIGH)


def spread(v, axis, dim, size):
    n = lax.axis_size(axis)
    me = lax.axis_index(axis)
    got = []
    for k in range(n):
        piece = lax.dynamic_slice_in_dim(v, lax.rem(me + k, n) * size, size, dim)
        if k > 0:
            piece = shift(piece, axis, k)
        got.append(piece)
    return got


def ring_gather(pieces, axis):
    below = [shift(v, axis, 1) for v in pieces]
    above = [shift(v, axis, -1) for v in pieces]
    far = []
    for k in range(4):
        far.append(shift((below if k < 2 else above)[k], axis, 1 if k < 2 else -1))
    return [pieces, below, far, above]


def split_kernel(core, err, mine, other):
    rows, chunks = mine.shape[1], err.shape[0] // mine.shape[1]
    per = mine.shape[2] // LANES
    for b in range(mine.shape[0]):
        for j in range(per):
            lanes = slice(j * LANES, (j + 1) * LANES)
            for out, half in ((mine, core[0]), (other, 1 - core[0])):
                out[b, :, lanes] = err[pl.ds(2 * per * b + per * half + j, rows, stride=chunks), :]


def split_error(err, core, chunks, side):
    rows = err.shape[0] // chunks
    step = 64
    shape = jax.ShapeDtypeStruct((4, rows, side // 2), F32)
    out = pl.BlockSpec((4, step, side // 2), lambda i, s: (0, i, 0))
    return pl.pallas_call(
        split_kernel,
        out_shape=(shape, shape),
        grid_spec=pltpu.PrefetchScalarGridSpec(
            num_scalar_prefetch=1,
            grid=(rows // step,),
            in_specs=[pl.BlockSpec((step * chunks, LANES), lambda i, s: (i, 0))],
            out_specs=(out, out),
        ),
        compiler_params=pltpu.CompilerParams(vmem_limit_bytes=24 * 2**20),
        cost_estimate=pl.CostEstimate(flops=10**6, bytes_accessed=8 * err.size, transcendentals=0),
    )(core, err)


def fold_kernel(x, mine, theirs, own, *sent):
    k = pl.program_id(0)
    total = mine[...] + theirs[...]

    @pl.when(k == 0)
    def _():
        own[...] = total

    for j, out in enumerate(sent):

        @pl.when(k == j + 1)
        def _(out=out):
            out[...] = total.astype(out.dtype)


def fold(x, mine, theirs, dtype):
    rows, width = mine.shape[0] // 4, mine.shape[1]
    taken = pl.BlockSpec((rows, width), lambda k, s: (lax.rem(s[0] + k, 4), 0))
    fixed = pl.BlockSpec((rows, width), lambda k, s: (0, 0))
    sent = jax.ShapeDtypeStruct((rows, width), dtype)
    parts = pl.pallas_call(
        fold_kernel,
        out_shape=(jax.ShapeDtypeStruct((rows, width), F32), sent, sent, sent),
        grid_spec=pltpu.PrefetchScalarGridSpec(
            num_scalar_prefetch=1, grid=(4,), in_specs=[taken, taken], out_specs=(fixed,) * 4
        ),
        compiler_params=pltpu.CompilerParams(vmem_limit_bytes=16 * 2**20),
        cost_estimate=pl.CostEstimate(flops=10**6, bytes_accessed=40 * rows * width, transcendentals=0),
    )(x.astype(jnp.int32).reshape(1), mine, theirs)
    return [parts[0]] + [shift(parts[k], "x", k) for k in (1, 2, 3)]


def pair_copies(n, refs, sa, sg, sems):
    toks = sa.shape[0] // n
    copies = []
    for i in range(n):
        rows = pl.ds(i * toks, toks)
        left = pltpu.make_async_copy(refs[i], sa.at[rows], sems.at[i])
        right = pltpu.make_async_copy(refs[n + i], sg.at[rows], sems.at[n + i])
        copies.append((left, right))
    return copies


def product(sa, sg, rows, lanes):
    dims = (((0,), (0,)), ((), ()))
    return lax.dot_general(sa[rows, lanes], sg[rows, :], dims, preferred_element_type=F32)


def block_rows(n, refs, sa, sg, sems, height, store):
    step = pl.program_id(0)
    toks = sa.shape[0] // n

    @pl.when(step == 0)
    def _():
        copies = pair_copies(n, refs, sa, sg, sems)
        for left, right in copies:
            left.start()
            right.start()
        total = None
        for low in range(0, n, 3):
            high = min(low + 3, n)
            for left, right in copies[low:high]:
                left.wait()
                right.wait()
            part = product(sa, sg, slice(low * toks, high * toks), slice(0, height))
            total = part if total is None else total + part
        store(total)

    @pl.when(step > 0)
    def _():
        lanes = pl.ds(pl.multiple_of(step * height, height), height)
        store(product(sa, sg, slice(0, n * toks), lanes))


def near_kernel(n, *refs):
    out, sa, sg, sems = refs[-4:]

    def store(total):
        out[...] = total

    block_rows(n, refs, sa, sg, sems, out.shape[0], store)


def rest_kernel(n, *refs):
    core, start, rounded, mine, other, sa, sg, sems = refs[-8:]
    half = mine.shape[1]

    def store(total):
        total = start[...] + total
        rounded[...] = total.astype(BF)
        first = core[0] == 0
        low, high = total[:, :half], total[:, half:]
        mine[...] = jnp.where(first, low, high)
        other[...] = jnp.where(first, high, low)

    block_rows(n, refs, sa, sg, sems, start.shape[0], store)


def block_call(kernel, pairs, a_all, g_all, extra, extra_specs, shapes):
    a = [a_all[m][k] for m, k in pairs]
    g = [g_all[k][m] for m, k in pairs]
    n, (toks, side) = len(pairs), a[0].shape
    moved = 4 * n * toks * side + 4 * side * side
    return pl.pallas_call(
        functools.partial(kernel, n),
        grid=(side // HEIGHT,),
        out_shape=shapes,
        in_specs=[pl.BlockSpec(memory_space=pl.ANY)] * (2 * n) + extra_specs,
        out_specs=jax.tree.map(lambda v: pl.BlockSpec((HEIGHT, v.shape[1]), lambda i: (i, 0)), shapes),
        scratch_shapes=[
            pltpu.VMEM((n * toks, side), BF),
            pltpu.VMEM((n * toks, side), BF),
            pltpu.SemaphoreType.DMA((2 * n,)),
        ],
        compiler_params=pltpu.CompilerParams(vmem_limit_bytes=32 * 2**20),
        cost_estimate=pl.CostEstimate(flops=2 * n * toks * side * side, bytes_accessed=moved, transcendentals=0),
    )(*a, *g, *extra)


def small_call(kernel, shapes, args, scalars=()):
    spec = pl.BlockSpec(memory_space=pltpu.VMEM)
    return pl.pallas_call(
        kernel,
        out_shape=shapes,
        in_specs=[pl.BlockSpec(memory_space=pltpu.SMEM)] * len(scalars) + [spec] * len(args),
        out_specs=jax.tree.map(lambda _: spec, shapes),
        compiler_params=pltpu.CompilerParams(vmem_limit_bytes=16 * 2**20),
        cost_estimate=pl.CostEstimate(flops=2 * 10**8, bytes_accessed=10**6, transcendentals=0),
    )(*scalars, *args)


def dot(a, b, dims):
    return lax.dot_general(a, b, (dims, ((), ())), precision=HIGH, preferred_element_type=F32)


def left_kernel(right, mean, out):
    out[...] = dot(right[...], mean[...], ((1,), (1,)))


def left_sum_kernel(own, far, below, above, mean, out, gram):
    half = mean.shape[1]
    right = (own[...] + far[...]) + (below[...] + above[...])
    out[...] = dot(right[:, :half], mean[...], ((1,), (1,)))
    gram[...] = right[:, half : half + LANES]


def right_kernel(scaled, *refs):
    if scaled:
        inv, own, far, below, above, mean, left_out, out = refs
    else:
        own, far, below, above, mean, left_out, out = refs
    left = (own[...] + far[...]) + (below[...] + above[...])
    if scaled:
        left = dot(inv[...], left, ((1,), (0,)))
    half = mean.shape[1]
    left_out[...] = left
    out[:, :half] = dot(left, mean[...], ((1,), (0,)))
    out[:, half:] = jnp.zeros((left.shape[0], LANES), F32)
    out[:, half : half + left.shape[0]] = dot(left, left, ((1,), (1,)))


def factor_kernel(place, inv, mine, theirs, factor, stacked):
    rank = inv.shape[0]
    half = mine.shape[1]
    y, core = place[0], place[1]
    for b in range(4):
        k = lax.rem(y - b + 4, 4)
        rows = pl.ds(pl.multiple_of(k * rank, rank), rank)
        ours, others = mine[rows, :], theirs[rows, :]
        for h in range(2):
            lanes = slice((2 * b + h) * half, (2 * b + h + 1) * half)
            value = dot(inv[...], jnp.where(core == h, ours, others), ((1,), (0,)))
            factor[:, lanes] = value
            hi = value.astype(BF)
            lo = (value - hi.astype(F32)).astype(BF)
            stacked[0:rank, lanes] = hi
            stacked[rank : 2 * rank, lanes] = lo
            stacked[2 * rank : 3 * rank, lanes] = hi


def ring(v, axis):
    return v, shift(v, axis, 2), shift(v, axis, 1), shift(v, axis, -1)


def after(v, token):
    return lax.optimization_barrier((v, token))[0]


def final_kernel(me, basis, factor, err, g0, g1, g2, g3, update, error_next):
    rows, chunks = basis.shape[0], factor.shape[1] // LANES
    per = g0.shape[1] // LANES
    for j in range(chunks):
        at, lanes = pl.ds(j, rows, stride=chunks), slice(j * LANES, (j + 1) * LANES)
        b, own = j // per, slice((j % per) * LANES, (j % per + 1) * LANES)
        k = lax.rem(me[0] - b + 4, 4)
        new = jnp.dot(basis[...], factor[:, lanes], preferred_element_type=F32)
        grad = jnp.where(
            k < 2,
            jnp.where(k == 0, g0[:, own].astype(F32), g1[:, own].astype(F32)),
            jnp.where(k == 2, g2[:, own].astype(F32), g3[:, own].astype(F32)),
        )
        update[at, :] = new
        error_next[at, :] = grad + err[at, :] - new


def basis_terms(basis):
    b = basis.T
    hi = lax.reduce_precision(b, 8, 7)
    return jnp.concatenate([hi, hi, b - hi], axis=1).astype(BF)


def finish(basis, right3, err, pieces):
    left3 = basis_terms(basis)
    own_rows, width = basis.shape[1], right3.shape[1]
    side = pieces[0].shape[1]
    step = 64
    chunks = width // LANES
    me = lax.axis_index("y").astype(jnp.int32).reshape(1)
    tall = pl.BlockSpec((step * chunks, LANES), lambda i, s: (i, 0))
    grads = pl.BlockSpec((step, side), lambda i, s: (i, 0))
    shape = jax.ShapeDtypeStruct((own_rows * chunks, LANES), F32)
    return pl.pallas_call(
        final_kernel,
        out_shape=(shape, shape),
        grid_spec=pltpu.PrefetchScalarGridSpec(
            num_scalar_prefetch=1,
            grid=(own_rows // step,),
            in_specs=[
                pl.BlockSpec((step, left3.shape[1]), lambda i, s: (i, 0)),
                pl.BlockSpec(right3.shape, lambda i, s: (0, 0)),
                tall,
                *[grads] * 4,
            ],
            out_specs=(tall, tall),
        ),
        compiler_params=pltpu.CompilerParams(vmem_limit_bytes=40 * 2**20),
        cost_estimate=pl.CostEstimate(flops=2 * 96 * own_rows * width, bytes_accessed=14 * own_rows * width, transcendentals=0),
    )(me, left3, right3, err, *pieces)


def inverse_kernel(gram, out):
    rank = gram.shape[0]
    row = lax.broadcasted_iota(jnp.int32, (rank, LANES), 0)
    lane = lax.broadcasted_iota(jnp.int32, (rank, LANES), 1)
    work = jnp.where(lane < rank, gram[...], jnp.where(lane == row + rank, 1.0, 0.0))
    for j in range(rank - 1):
        pivot = work[j : j + 1, :]
        ratio = jnp.where(row > j, work[:, j : j + 1] / work[j : j + 1, j : j + 1], 0.0)
        work = work - ratio * pivot
    scale = jnp.sum(jnp.where(lane == row, work, 0.0), axis=1, keepdims=True)
    out[...] = work[:, rank : 2 * rank] / jnp.sqrt(scale)


def inverse_factor(gram):
    rank = gram.shape[0]
    return small_call(inverse_kernel, jax.ShapeDtypeStruct((rank, rank), F32), (gram,))


def local(activations, out_grads, error, q_start):
    acts, grads = activations[0], out_grads[0]
    _, width = acts.shape
    own_rows = error.shape[1]
    rank = q_start.shape[1]
    groups = lax.axis_size(GRP)
    side, half = width // 4, width // 8
    chunks = width // LANES
    x, core, y = lax.axis_index("x"), lax.axis_index("c"), lax.axis_index("y")
    core_ref = core.astype(jnp.int32).reshape(1)

    a_own = spread(acts, "z", 1, side)
    g_own = spread(grads, "y", 1, side)
    a_all = ring_gather(a_own, "y")
    g_all = ring_gather(g_own, "z")

    err = error.reshape(own_rows * chunks, LANES)
    mine, other = split_error(err, core_ref, chunks, side)
    other = shift(other, "c", 1).reshape(4 * own_rows, half)
    parts = fold(x, mine.reshape(4 * own_rows, half), other, F32)
    mean = swapped((parts[0] + parts[1]) + (parts[2] + parts[3]))

    seen = [(m, k) for m in (0, 1, 3) for k in (0, 1, 3)]
    rest = [(2, k) for k in range(4)] + [(m, 2) for m in (0, 1, 3)]
    whole = jax.ShapeDtypeStruct((side, side), F32)
    part = jax.ShapeDtypeStruct((side, half), F32)
    smem = pl.BlockSpec(memory_space=pltpu.SMEM)
    block = pl.BlockSpec((HEIGHT, side), lambda i: (i, 0))
    near = block_call(near_kernel, seen, a_all, g_all, [], [], whole)
    rounded, mine, other = block_call(
        rest_kernel, rest, a_all, g_all, [core_ref, near], [smem, block],
        (jax.ShapeDtypeStruct((side, side), BF), part, part),
    )
    parts = fold(x, mine, shift(other, "c", 1), BF)
    pieces = [lax.dynamic_slice_in_dim(rounded, lax.rem(y + k, 4) * own_rows, own_rows, 0) for k in range(4)]
    pieces[1], pieces[3] = shift(pieces[1], "y", 1), shift(pieces[3], "y", 3)
    mean = ((mean + parts[0]) + (parts[1].astype(F32) + parts[2].astype(F32)) + parts[3].astype(F32)) / groups

    right = lax.dynamic_slice_in_dim(q_start[0], y * side + core * half, half, 1)
    left_shape = jax.ShapeDtypeStruct((rank, own_rows), F32)
    right_shape = jax.ShapeDtypeStruct((rank, half + LANES), F32)
    gram_shape = jax.ShapeDtypeStruct((rank, LANES), F32)
    partial = small_call(left_kernel, left_shape, (right, mean))
    for step in range(ITERS):
        partial = partial + shift(partial, "c", 1)
        if step == 0:
            partial, pieces[1], pieces[3] = lax.optimization_barrier((partial, pieces[1], pieces[3]))
            terms = (*ring(partial, "y"), mean)
        else:
            partial, pieces[2] = lax.optimization_barrier((partial, pieces[2]))
            terms = (inverse_factor(gram), *ring(partial, "y"), mean)
        left, both = small_call(functools.partial(right_kernel, step > 0), (left_shape, right_shape), terms)
        if step == 0:
            pieces[2] = shift(after(pieces[2], both), "y", 2)
        own, far, below, above = ring(both, "z")
        both = (own + far) + (below + above)
        if step + 1 < ITERS:
            partial, gram = small_call(left_sum_kernel, (left_shape, gram_shape), (*ring(both, "x"), mean))
    own, far, below, above = ring(both, "x")
    both = (own + far) + (below + above)
    right, gram = both[:, :half], both[:, half:]
    inv = inverse_factor(gram)
    got = jnp.concatenate([right] + [shift(right, "y", k) for k in (1, 2, 3)], axis=0)
    place = jnp.stack([y, core]).astype(jnp.int32)
    right, stacked = small_call(
        factor_kernel,
        (jax.ShapeDtypeStruct((rank, width), F32), jax.ShapeDtypeStruct((3 * rank, width), BF)),
        (inv, got, shift(got, "c", 1)),
        (place,),
    )
    basis = times(inv, swapped(left), ((1,), (0,)))
    update, error_next = finish(basis, stacked, err, pieces)
    return (
        update.reshape(own_rows, 1, width),
        error_next.reshape(1, own_rows, 1, width),
        right[None],
    )


def solution(mesh):
    split = Mesh(mesh.devices.reshape(4, 2, 4, 4), ALL)

    return jax.shard_map(
        local,
        mesh=split,
        in_specs=(
            P(None, ALL, None),
            P(None, ALL, None),
            P(GRP, SHARD, None, None),
            P(),
        ),
        out_specs=(P(SHARD, None, None), P(GRP, SHARD, None, None), P()),
        check_vma=False,
    )
```

```python
import functools

import jax
import jax.numpy as jnp
from jax import lax
from jax.experimental import pallas as pl
from jax.experimental.pallas import tpu as pltpu
from jax.sharding import Mesh
from jax.sharding import PartitionSpec as P

GRP = ("x", "c")
SHARD = ("z", "y")
ALL = ("x", "c", "z", "y")
BF = jnp.bfloat16
F32 = jnp.float32
HIGH = lax.Precision.HIGHEST
ITERS = 2
LANES = 128
HEIGHT = 256
FULL = 60 * 2**20


def shift(v, axis, by):
    n = lax.axis_size(axis)
    return lax.ppermute(v, axis, [(i, (i + by) % n) for i in range(n)])


def swapped(v):
    n = lax.axis_size("x")
    pairs = [(i * n + j, j * n + i) for i in range(n) for j in range(n)]
    return lax.ppermute(v, ("x", "y"), pairs)


def times(a, b, dims):
    return lax.dot_general(a, b, (dims, ((), ())), precision=HIGH)


def spread(v, axis, dim, size):
    n = lax.axis_size(axis)
    me = lax.axis_index(axis)
    got = []
    for k in range(n):
        piece = lax.dynamic_slice_in_dim(v, lax.rem(me + k, n) * size, size, dim)
        if k > 0:
            piece = shift(piece, axis, k)
        got.append(piece)
    return got


def ring_gather(pieces, axis):
    below = [shift(v, axis, 1) for v in pieces]
    above = [shift(v, axis, -1) for v in pieces]
    far = []
    for k in range(4):
        far.append(shift((below if k < 2 else above)[k], axis, 1 if k < 2 else -1))
    return [pieces, below, far, above]


def split_kernel(core, err, mine, other):
    rows, chunks = mine.shape[1], err.shape[0] // mine.shape[1]
    per = mine.shape[2] // LANES
    for b in range(mine.shape[0]):
        for j in range(per):
            lanes = slice(j * LANES, (j + 1) * LANES)
            for out, half in ((mine, core[0]), (other, 1 - core[0])):
                out[b, :, lanes] = err[pl.ds(2 * per * b + per * half + j, rows, stride=chunks), :]


def split_error(err, core, chunks, side):
    rows = err.shape[0] // chunks
    step = 64
    shape = jax.ShapeDtypeStruct((4, rows, side // 2), F32)
    out = pl.BlockSpec((4, step, side // 2), lambda i, s: (0, i, 0))
    return pl.pallas_call(
        split_kernel,
        out_shape=(shape, shape),
        grid_spec=pltpu.PrefetchScalarGridSpec(
            num_scalar_prefetch=1,
            grid=(rows // step,),
            in_specs=[pl.BlockSpec((step * chunks, LANES), lambda i, s: (i, 0))],
            out_specs=(out, out),
        ),
        compiler_params=pltpu.CompilerParams(vmem_limit_bytes=FULL),
        cost_estimate=pl.CostEstimate(flops=10**6, bytes_accessed=8 * err.size, transcendentals=0),
    )(core, err)


def fold_kernel(x, mine, theirs, own, *sent):
    k = pl.program_id(0)
    total = mine[...] + theirs[...]

    @pl.when(k == 0)
    def _():
        own[...] = total

    for j, out in enumerate(sent):

        @pl.when(k == j + 1)
        def _(out=out):
            out[...] = total.astype(out.dtype)


def fold(x, mine, theirs, dtype):
    rows, width = mine.shape[0] // 4, mine.shape[1]
    taken = pl.BlockSpec((rows, width), lambda k, s: (lax.rem(s[0] + k, 4), 0))
    fixed = pl.BlockSpec((rows, width), lambda k, s: (0, 0))
    sent = jax.ShapeDtypeStruct((rows, width), dtype)
    parts = pl.pallas_call(
        fold_kernel,
        out_shape=(jax.ShapeDtypeStruct((rows, width), F32), sent, sent, sent),
        grid_spec=pltpu.PrefetchScalarGridSpec(
            num_scalar_prefetch=1, grid=(4,), in_specs=[taken, taken], out_specs=(fixed,) * 4
        ),
        compiler_params=pltpu.CompilerParams(vmem_limit_bytes=FULL),
        cost_estimate=pl.CostEstimate(flops=10**6, bytes_accessed=40 * rows * width, transcendentals=0),
    )(x.astype(jnp.int32).reshape(1), mine, theirs)
    return [parts[0]] + [shift(parts[k], "x", k) for k in (1, 2, 3)]


def pair_copies(n, refs, sa, sg, sems):
    toks = sa.shape[0] // n
    copies = []
    for i in range(n):
        rows = pl.ds(i * toks, toks)
        left = pltpu.make_async_copy(refs[i], sa.at[rows], sems.at[i])
        right = pltpu.make_async_copy(refs[n + i], sg.at[rows], sems.at[n + i])
        copies.append((left, right))
    return copies


def product(sa, sg, rows, lanes):
    dims = (((0,), (0,)), ((), ()))
    return lax.dot_general(sa[rows, lanes], sg[rows, :], dims, preferred_element_type=F32)


def block_rows(n, refs, sa, sg, sems, height, store):
    step = pl.program_id(0)
    toks = sa.shape[0] // n

    @pl.when(step == 0)
    def _():
        copies = pair_copies(n, refs, sa, sg, sems)
        for left, right in copies:
            left.start()
            right.start()
        total = None
        for low in range(0, n, 3):
            high = min(low + 3, n)
            for left, right in copies[low:high]:
                left.wait()
                right.wait()
            part = product(sa, sg, slice(low * toks, high * toks), slice(0, height))
            total = part if total is None else total + part
        store(total)

    @pl.when(step > 0)
    def _():
        lanes = pl.ds(pl.multiple_of(step * height, height), height)
        store(product(sa, sg, slice(0, n * toks), lanes))


def near_kernel(n, *refs):
    out, sa, sg, sems = refs[-4:]

    def store(total):
        out[...] = total

    block_rows(n, refs, sa, sg, sems, out.shape[0], store)


def middle_kernel(n, *refs):
    start, out, sa, sg, sems = refs[-5:]

    def store(total):
        out[...] = start[...] + total

    block_rows(n, refs, sa, sg, sems, out.shape[0], store)


def rest_kernel(n, *refs):
    core, start, rounded, mine, other, sa, sg, sems = refs[-8:]
    half = mine.shape[1]

    def store(total):
        total = start[...] + total
        rounded[...] = total.astype(BF)
        first = core[0] == 0
        low, high = total[:, :half], total[:, half:]
        mine[...] = jnp.where(first, low, high)
        other[...] = jnp.where(first, high, low)

    block_rows(n, refs, sa, sg, sems, start.shape[0], store)


def block_call(kernel, pairs, a_all, g_all, extra, extra_specs, shapes):
    a = [a_all[m][k] for m, k in pairs]
    g = [g_all[k][m] for m, k in pairs]
    n, (toks, side) = len(pairs), a[0].shape
    moved = 4 * n * toks * side + 4 * side * side
    return pl.pallas_call(
        functools.partial(kernel, n),
        grid=(side // HEIGHT,),
        out_shape=shapes,
        in_specs=[pl.BlockSpec(memory_space=pl.ANY)] * (2 * n) + extra_specs,
        out_specs=jax.tree.map(lambda v: pl.BlockSpec((HEIGHT, v.shape[1]), lambda i: (i, 0)), shapes),
        scratch_shapes=[
            pltpu.VMEM((n * toks, side), BF),
            pltpu.VMEM((n * toks, side), BF),
            pltpu.SemaphoreType.DMA((2 * n,)),
        ],
        compiler_params=pltpu.CompilerParams(vmem_limit_bytes=FULL),
        cost_estimate=pl.CostEstimate(flops=2 * n * toks * side * side, bytes_accessed=moved, transcendentals=0),
    )(*a, *g, *extra)


def small_call(kernel, shapes, args, scalars=()):
    spec = pl.BlockSpec(memory_space=pltpu.VMEM)
    return pl.pallas_call(
        kernel,
        out_shape=shapes,
        in_specs=[pl.BlockSpec(memory_space=pltpu.SMEM)] * len(scalars) + [spec] * len(args),
        out_specs=jax.tree.map(lambda _: spec, shapes),
        compiler_params=pltpu.CompilerParams(vmem_limit_bytes=16 * 2**20),
        cost_estimate=pl.CostEstimate(flops=2 * 10**8, bytes_accessed=10**6, transcendentals=0),
    )(*scalars, *args)


def dot(a, b, dims):
    return lax.dot_general(a, b, (dims, ((), ())), precision=HIGH, preferred_element_type=F32)


def left_kernel(right, mean, out):
    out[...] = dot(right[...], mean[...], ((1,), (1,)))


def left_sum_kernel(own, far, below, above, mean, out, gram):
    half = mean.shape[1]
    right = (own[...] + far[...]) + (below[...] + above[...])
    out[...] = dot(right[:, :half], mean[...], ((1,), (1,)))
    gram[...] = right[:, half : half + LANES]


def right_kernel(scaled, *refs):
    if scaled:
        inv, own, far, below, above, mean, left_out, out = refs
    else:
        own, far, below, above, mean, left_out, out = refs
    left = (own[...] + far[...]) + (below[...] + above[...])
    if scaled:
        left = dot(inv[...], left, ((1,), (0,)))
    half = mean.shape[1]
    left_out[...] = left
    out[:, :half] = dot(left, mean[...], ((1,), (0,)))
    out[:, half:] = jnp.zeros((left.shape[0], LANES), F32)
    out[:, half : half + left.shape[0]] = dot(left, left, ((1,), (1,)))


def factor_kernel(place, inv, mine, theirs, factor, stacked):
    rank = inv.shape[0]
    half = mine.shape[1]
    y, core = place[0], place[1]
    for b in range(4):
        k = lax.rem(y - b + 4, 4)
        rows = pl.ds(pl.multiple_of(k * rank, rank), rank)
        ours, others = mine[rows, :], theirs[rows, :]
        for h in range(2):
            lanes = slice((2 * b + h) * half, (2 * b + h + 1) * half)
            value = dot(inv[...], jnp.where(core == h, ours, others), ((1,), (0,)))
            factor[:, lanes] = value
            hi = value.astype(BF)
            lo = (value - hi.astype(F32)).astype(BF)
            stacked[0:rank, lanes] = hi
            stacked[rank : 2 * rank, lanes] = lo
            stacked[2 * rank : 3 * rank, lanes] = hi


def ring(v, axis):
    return v, shift(v, axis, 2), shift(v, axis, 1), shift(v, axis, -1)


def after(v, token):
    return lax.optimization_barrier((v, token))[0]


def final_kernel(me, basis, factor, err, g0, g1, g2, g3, update, error_next):
    rows, chunks = basis.shape[0], factor.shape[1] // LANES
    per = g0.shape[1] // LANES
    for j in range(chunks):
        at, lanes = pl.ds(j, rows, stride=chunks), slice(j * LANES, (j + 1) * LANES)
        b, own = j // per, slice((j % per) * LANES, (j % per + 1) * LANES)
        k = lax.rem(me[0] - b + 4, 4)
        new = jnp.dot(basis[...], factor[:, lanes], preferred_element_type=F32)
        grad = jnp.where(
            k < 2,
            jnp.where(k == 0, g0[:, own].astype(F32), g1[:, own].astype(F32)),
            jnp.where(k == 2, g2[:, own].astype(F32), g3[:, own].astype(F32)),
        )
        update[at, :] = new
        error_next[at, :] = grad + err[at, :] - new


def basis_terms(basis):
    b = basis.T
    hi = lax.reduce_precision(b, 8, 7)
    return jnp.concatenate([hi, hi, b - hi], axis=1).astype(BF)


def finish(basis, right3, err, pieces):
    left3 = basis_terms(basis)
    own_rows, width = basis.shape[1], right3.shape[1]
    side = pieces[0].shape[1]
    step = 64
    chunks = width // LANES
    me = lax.axis_index("y").astype(jnp.int32).reshape(1)
    tall = pl.BlockSpec((step * chunks, LANES), lambda i, s: (i, 0))
    grads = pl.BlockSpec((step, side), lambda i, s: (i, 0))
    shape = jax.ShapeDtypeStruct((own_rows * chunks, LANES), F32)
    return pl.pallas_call(
        final_kernel,
        out_shape=(shape, shape),
        grid_spec=pltpu.PrefetchScalarGridSpec(
            num_scalar_prefetch=1,
            grid=(own_rows // step,),
            in_specs=[
                pl.BlockSpec((step, left3.shape[1]), lambda i, s: (i, 0)),
                pl.BlockSpec(right3.shape, lambda i, s: (0, 0)),
                tall,
                *[grads] * 4,
            ],
            out_specs=(tall, tall),
        ),
        compiler_params=pltpu.CompilerParams(vmem_limit_bytes=FULL),
        cost_estimate=pl.CostEstimate(flops=2 * 96 * own_rows * width, bytes_accessed=14 * own_rows * width, transcendentals=0),
    )(me, left3, right3, err, *pieces)


def inverse_kernel(gram, out):
    rank = gram.shape[0]
    row = lax.broadcasted_iota(jnp.int32, (rank, LANES), 0)
    lane = lax.broadcasted_iota(jnp.int32, (rank, LANES), 1)
    work = jnp.where(lane < rank, gram[...], jnp.where(lane == row + rank, 1.0, 0.0))
    for j in range(rank - 1):
        pivot = work[j : j + 1, :]
        ratio = jnp.where(row > j, work[:, j : j + 1] / work[j : j + 1, j : j + 1], 0.0)
        work = work - ratio * pivot
    scale = jnp.sum(jnp.where(lane == row, work, 0.0), axis=1, keepdims=True)
    out[...] = work[:, rank : 2 * rank] / jnp.sqrt(scale)


def inverse_factor(gram):
    rank = gram.shape[0]
    return small_call(inverse_kernel, jax.ShapeDtypeStruct((rank, rank), F32), (gram,))


def local(activations, out_grads, error, q_start):
    acts, grads = activations[0], out_grads[0]
    _, width = acts.shape
    own_rows = error.shape[1]
    rank = q_start.shape[1]
    groups = lax.axis_size(GRP)
    side, half = width // 4, width // 8
    chunks = width // LANES
    x, core, y = lax.axis_index("x"), lax.axis_index("c"), lax.axis_index("y")
    core_ref = core.astype(jnp.int32).reshape(1)

    a_own = spread(acts, "z", 1, side)
    g_own = spread(grads, "y", 1, side)
    a_all = ring_gather(a_own, "y")
    g_all = ring_gather(g_own, "z")

    err = error.reshape(own_rows * chunks, LANES)
    mine, other = split_error(err, core_ref, chunks, side)
    other = shift(other, "c", 1).reshape(4 * own_rows, half)
    parts = fold(x, mine.reshape(4 * own_rows, half), other, F32)
    mean = swapped((parts[0] + parts[1]) + (parts[2] + parts[3]))

    seen = [(m, k) for m in (0, 1, 3) for k in (0, 1, 3)]
    middle = [(2, 0), (0, 2), (2, 2)]
    rest = [(2, 1), (1, 2), (2, 3), (3, 2)]
    whole = jax.ShapeDtypeStruct((side, side), F32)
    part = jax.ShapeDtypeStruct((side, half), F32)
    smem = pl.BlockSpec(memory_space=pltpu.SMEM)
    block = pl.BlockSpec((HEIGHT, side), lambda i: (i, 0))
    near = block_call(near_kernel, seen, a_all, g_all, [], [], whole)
    near = block_call(middle_kernel, middle, a_all, g_all, [near], [block], whole)
    rounded, mine, other = block_call(
        rest_kernel, rest, a_all, g_all, [core_ref, near], [smem, block],
        (jax.ShapeDtypeStruct((side, side), BF), part, part),
    )
    parts = fold(x, mine, shift(other, "c", 1), BF)
    pieces = [lax.dynamic_slice_in_dim(rounded, lax.rem(y + k, 4) * own_rows, own_rows, 0) for k in range(4)]
    pieces[1], pieces[3] = shift(pieces[1], "y", 1), shift(pieces[3], "y", 3)
    mean = ((mean + parts[0]) + (parts[1].astype(F32) + parts[2].astype(F32)) + parts[3].astype(F32)) / groups

    right = lax.dynamic_slice_in_dim(q_start[0], y * side + core * half, half, 1)
    left_shape = jax.ShapeDtypeStruct((rank, own_rows), F32)
    right_shape = jax.ShapeDtypeStruct((rank, half + LANES), F32)
    gram_shape = jax.ShapeDtypeStruct((rank, LANES), F32)
    partial = small_call(left_kernel, left_shape, (right, mean))
    for step in range(ITERS):
        partial = partial + shift(partial, "c", 1)
        if step == 0:
            partial, pieces[1], pieces[3] = lax.optimization_barrier((partial, pieces[1], pieces[3]))
            terms = (*ring(partial, "y"), mean)
        else:
            partial, pieces[2] = lax.optimization_barrier((partial, pieces[2]))
            terms = (inverse_factor(gram), *ring(partial, "y"), mean)
        left, both = small_call(functools.partial(right_kernel, step > 0), (left_shape, right_shape), terms)
        if step == 0:
            pieces[2] = shift(after(pieces[2], both), "y", 2)
        own, far, below, above = ring(both, "z")
        both = (own + far) + (below + above)
        if step + 1 < ITERS:
            partial, gram = small_call(left_sum_kernel, (left_shape, gram_shape), (*ring(both, "x"), mean))
    own, far, below, above = ring(both, "x")
    both = (own + far) + (below + above)
    right, gram = both[:, :half], both[:, half:]
    inv = inverse_factor(gram)
    got = jnp.concatenate([right] + [shift(right, "y", k) for k in (1, 2, 3)], axis=0)
    place = jnp.stack([y, core]).astype(jnp.int32)
    right, stacked = small_call(
        factor_kernel,
        (jax.ShapeDtypeStruct((rank, width), F32), jax.ShapeDtypeStruct((3 * rank, width), BF)),
        (inv, got, shift(got, "c", 1)),
        (place,),
    )
    basis = times(inv, swapped(left), ((1,), (0,)))
    update, error_next = finish(basis, stacked, err, pieces)
    return (
        update.reshape(own_rows, 1, width),
        error_next.reshape(1, own_rows, 1, width),
        right[None],
    )


def solution(mesh):
    split = Mesh(mesh.devices.reshape(4, 2, 4, 4), ALL)

    return jax.shard_map(
        local,
        mesh=split,
        in_specs=(
            P(None, ALL, None),
            P(None, ALL, None),
            P(GRP, SHARD, None, None),
            P(),
        ),
        out_specs=(P(SHARD, None, None), P(GRP, SHARD, None, None), P()),
        check_vma=False,
    )
```

```python
import functools

import jax
import jax.numpy as jnp
from jax import lax
from jax.experimental import pallas as pl
from jax.experimental.pallas import tpu as pltpu
from jax.sharding import Mesh
from jax.sharding import PartitionSpec as P

GRP = ("x", "c")
SHARD = ("z", "y")
ALL = ("x", "c", "z", "y")
BF = jnp.bfloat16
F32 = jnp.float32
HIGH = lax.Precision.HIGHEST
ITERS = 2
LANES = 128
HEIGHT = 256
FULL = 60 * 2**20


def shift(v, axis, by):
    n = lax.axis_size(axis)
    return lax.ppermute(v, axis, [(i, (i + by) % n) for i in range(n)])


def swapped(v):
    n = lax.axis_size("x")
    pairs = [(i * n + j, j * n + i) for i in range(n) for j in range(n)]
    return lax.ppermute(v, ("x", "y"), pairs)


def times(a, b, dims):
    return lax.dot_general(a, b, (dims, ((), ())), precision=HIGH)


def spread(v, axis, dim, size):
    n = lax.axis_size(axis)
    me = lax.axis_index(axis)
    got = []
    for k in range(n):
        piece = lax.dynamic_slice_in_dim(v, lax.rem(me + k, n) * size, size, dim)
        if k > 0:
            piece = shift(piece, axis, k)
        got.append(piece)
    return got


def ring_gather(pieces, axis):
    below = [shift(v, axis, 1) for v in pieces]
    above = [shift(v, axis, -1) for v in pieces]
    far = []
    for k in range(4):
        far.append(shift((below if k < 2 else above)[k], axis, 1 if k < 2 else -1))
    return [pieces, below, far, above]


def split_kernel(core, err, mine, other):
    rows, chunks = mine.shape[1], err.shape[0] // mine.shape[1]
    per = mine.shape[2] // LANES
    for b in range(mine.shape[0]):
        for j in range(per):
            lanes = slice(j * LANES, (j + 1) * LANES)
            for out, half in ((mine, core[0]), (other, 1 - core[0])):
                out[b, :, lanes] = err[pl.ds(2 * per * b + per * half + j, rows, stride=chunks), :]


def split_error(err, core, chunks, side):
    rows = err.shape[0] // chunks
    step = 64
    shape = jax.ShapeDtypeStruct((4, rows, side // 2), F32)
    out = pl.BlockSpec((4, step, side // 2), lambda i, s: (0, i, 0))
    return pl.pallas_call(
        split_kernel,
        out_shape=(shape, shape),
        grid_spec=pltpu.PrefetchScalarGridSpec(
            num_scalar_prefetch=1,
            grid=(rows // step,),
            in_specs=[pl.BlockSpec((step * chunks, LANES), lambda i, s: (i, 0))],
            out_specs=(out, out),
        ),
        compiler_params=pltpu.CompilerParams(vmem_limit_bytes=FULL),
        cost_estimate=pl.CostEstimate(flops=10**6, bytes_accessed=8 * err.size, transcendentals=0),
    )(core, err)


def fold_kernel(x, mine, theirs, own, *sent):
    k = pl.program_id(0)
    total = mine[...] + theirs[...]

    @pl.when(k == 0)
    def _():
        own[...] = total

    for j, out in enumerate(sent):

        @pl.when(k == j + 1)
        def _(out=out):
            out[...] = total.astype(out.dtype)


def fold(x, mine, theirs, dtype):
    rows, width = mine.shape[0] // 4, mine.shape[1]
    taken = pl.BlockSpec((rows, width), lambda k, s: (lax.rem(s[0] + k, 4), 0))
    fixed = pl.BlockSpec((rows, width), lambda k, s: (0, 0))
    sent = jax.ShapeDtypeStruct((rows, width), dtype)
    parts = pl.pallas_call(
        fold_kernel,
        out_shape=(jax.ShapeDtypeStruct((rows, width), F32), sent, sent, sent),
        grid_spec=pltpu.PrefetchScalarGridSpec(
            num_scalar_prefetch=1, grid=(4,), in_specs=[taken, taken], out_specs=(fixed,) * 4
        ),
        compiler_params=pltpu.CompilerParams(vmem_limit_bytes=FULL),
        cost_estimate=pl.CostEstimate(flops=10**6, bytes_accessed=40 * rows * width, transcendentals=0),
    )(x.astype(jnp.int32).reshape(1), mine, theirs)
    return [parts[0]] + [shift(parts[k], "x", k) for k in (1, 2, 3)]


def pair_copies(n, refs, sa, sg, sems):
    toks = sa.shape[0] // n
    copies = []
    for i in range(n):
        rows = pl.ds(i * toks, toks)
        left = pltpu.make_async_copy(refs[i], sa.at[rows], sems.at[i])
        right = pltpu.make_async_copy(refs[n + i], sg.at[rows], sems.at[n + i])
        copies.append((left, right))
    return copies


def product(sa, sg, rows, lanes):
    dims = (((0,), (0,)), ((), ()))
    return lax.dot_general(sa[rows, lanes], sg[rows, :], dims, preferred_element_type=F32)


def block_rows(n, refs, sa, sg, sems, height, store):
    step = pl.program_id(0)
    toks = sa.shape[0] // n

    @pl.when(step == 0)
    def _():
        copies = pair_copies(n, refs, sa, sg, sems)
        for left, right in copies:
            left.start()
            right.start()
        total = None
        for low in range(0, n, 3):
            high = min(low + 3, n)
            for left, right in copies[low:high]:
                left.wait()
                right.wait()
            part = product(sa, sg, slice(low * toks, high * toks), slice(0, height))
            total = part if total is None else total + part
        store(total)

    @pl.when(step > 0)
    def _():
        lanes = pl.ds(pl.multiple_of(step * height, height), height)
        store(product(sa, sg, slice(0, n * toks), lanes))


def near_kernel(n, *refs):
    out, sa, sg, sems = refs[-4:]

    def store(total):
        out[...] = total

    block_rows(n, refs, sa, sg, sems, out.shape[0], store)


def rest_kernel(n, *refs):
    core, start, rounded, mine, other, sa, sg, sems = refs[-8:]
    half = mine.shape[1]

    def store(total):
        total = start[...] + total
        rounded[...] = total.astype(BF)
        first = core[0] == 0
        low, high = total[:, :half], total[:, half:]
        mine[...] = jnp.where(first, low, high)
        other[...] = jnp.where(first, high, low)

    block_rows(n, refs, sa, sg, sems, start.shape[0], store)


def block_call(kernel, pairs, a_all, g_all, extra, extra_specs, shapes):
    a = [a_all[m][k] for m, k in pairs]
    g = [g_all[k][m] for m, k in pairs]
    n, (toks, side) = len(pairs), a[0].shape
    moved = 4 * n * toks * side + 4 * side * side
    return pl.pallas_call(
        functools.partial(kernel, n),
        grid=(side // HEIGHT,),
        out_shape=shapes,
        in_specs=[pl.BlockSpec(memory_space=pl.ANY)] * (2 * n) + extra_specs,
        out_specs=jax.tree.map(lambda v: pl.BlockSpec((HEIGHT, v.shape[1]), lambda i: (i, 0)), shapes),
        scratch_shapes=[
            pltpu.VMEM((n * toks, side), BF),
            pltpu.VMEM((n * toks, side), BF),
            pltpu.SemaphoreType.DMA((2 * n,)),
        ],
        compiler_params=pltpu.CompilerParams(vmem_limit_bytes=FULL),
        cost_estimate=pl.CostEstimate(flops=2 * n * toks * side * side, bytes_accessed=moved, transcendentals=0),
    )(*a, *g, *extra)


def small_call(kernel, shapes, args, scalars=()):
    spec = pl.BlockSpec(memory_space=pltpu.VMEM)
    return pl.pallas_call(
        kernel,
        out_shape=shapes,
        in_specs=[pl.BlockSpec(memory_space=pltpu.SMEM)] * len(scalars) + [spec] * len(args),
        out_specs=jax.tree.map(lambda _: spec, shapes),
        compiler_params=pltpu.CompilerParams(vmem_limit_bytes=16 * 2**20),
        cost_estimate=pl.CostEstimate(flops=2 * 10**8, bytes_accessed=10**6, transcendentals=0),
    )(*scalars, *args)


def dot(a, b, dims):
    return lax.dot_general(a, b, (dims, ((), ())), precision=HIGH, preferred_element_type=F32)


def left_kernel(right, mean, out):
    out[...] = dot(right[...], mean[...], ((1,), (1,)))


def left_sum_kernel(own, far, below, above, mean, out, gram):
    half = mean.shape[1]
    right = (own[...] + far[...]) + (below[...] + above[...])
    out[...] = dot(right[:, :half], mean[...], ((1,), (1,)))
    gram[...] = right[:, half : half + LANES]


def right_kernel(scaled, *refs):
    if scaled:
        inv, own, far, below, above, mean, left_out, out = refs
    else:
        own, far, below, above, mean, left_out, out = refs
    left = (own[...] + far[...]) + (below[...] + above[...])
    if scaled:
        left = dot(inv[...], left, ((1,), (0,)))
    half = mean.shape[1]
    left_out[...] = left
    out[:, :half] = dot(left, mean[...], ((1,), (0,)))
    out[:, half:] = jnp.zeros((left.shape[0], LANES), F32)
    out[:, half : half + left.shape[0]] = dot(left, left, ((1,), (1,)))


def factor_kernel(place, inv, mine, theirs, factor, stacked):
    rank = inv.shape[0]
    half = mine.shape[1]
    y, core = place[0], place[1]
    for b in range(4):
        k = lax.rem(y - b + 4, 4)
        rows = pl.ds(pl.multiple_of(k * rank, rank), rank)
        ours, others = mine[rows, :], theirs[rows, :]
        for h in range(2):
            lanes = slice((2 * b + h) * half, (2 * b + h + 1) * half)
            value = dot(inv[...], jnp.where(core == h, ours, others), ((1,), (0,)))
            factor[:, lanes] = value
            hi = value.astype(BF)
            lo = (value - hi.astype(F32)).astype(BF)
            stacked[0:rank, lanes] = hi
            stacked[rank : 2 * rank, lanes] = lo
            stacked[2 * rank : 3 * rank, lanes] = hi


def ring(v, axis):
    return v, shift(v, axis, 2), shift(v, axis, 1), shift(v, axis, -1)


def after(v, token):
    return lax.optimization_barrier((v, token))[0]


def final_kernel(me, basis, factor, err, g0, g1, g2, g3, update, error_next):
    rows, chunks = basis.shape[0], factor.shape[1] // LANES
    per = g0.shape[1] // LANES
    for j in range(chunks):
        at, lanes = pl.ds(j, rows, stride=chunks), slice(j * LANES, (j + 1) * LANES)
        b, own = j // per, slice((j % per) * LANES, (j % per + 1) * LANES)
        k = lax.rem(me[0] - b + 4, 4)
        new = jnp.dot(basis[...], factor[:, lanes], preferred_element_type=F32)
        grad = jnp.where(
            k < 2,
            jnp.where(k == 0, g0[:, own].astype(F32), g1[:, own].astype(F32)),
            jnp.where(k == 2, g2[:, own].astype(F32), g3[:, own].astype(F32)),
        )
        update[at, :] = new
        error_next[at, :] = grad + err[at, :] - new


def basis_terms(basis):
    b = basis.T
    hi = lax.reduce_precision(b, 8, 7)
    return jnp.concatenate([hi, hi, b - hi], axis=1).astype(BF)


def finish(basis, right3, err, pieces):
    left3 = basis_terms(basis)
    own_rows, width = basis.shape[1], right3.shape[1]
    side = pieces[0].shape[1]
    step = 64
    chunks = width // LANES
    me = lax.axis_index("y").astype(jnp.int32).reshape(1)
    tall = pl.BlockSpec((step * chunks, LANES), lambda i, s: (i, 0))
    grads = pl.BlockSpec((step, side), lambda i, s: (i, 0))
    shape = jax.ShapeDtypeStruct((own_rows * chunks, LANES), F32)
    return pl.pallas_call(
        final_kernel,
        out_shape=(shape, shape),
        grid_spec=pltpu.PrefetchScalarGridSpec(
            num_scalar_prefetch=1,
            grid=(own_rows // step,),
            in_specs=[
                pl.BlockSpec((step, left3.shape[1]), lambda i, s: (i, 0)),
                pl.BlockSpec(right3.shape, lambda i, s: (0, 0)),
                tall,
                *[grads] * 4,
            ],
            out_specs=(tall, tall),
        ),
        compiler_params=pltpu.CompilerParams(vmem_limit_bytes=FULL),
        cost_estimate=pl.CostEstimate(flops=2 * 96 * own_rows * width, bytes_accessed=14 * own_rows * width, transcendentals=0),
    )(me, left3, right3, err, *pieces)


def inverse_kernel(gram, out):
    rank = gram.shape[0]
    row = lax.broadcasted_iota(jnp.int32, (rank, LANES), 0)
    lane = lax.broadcasted_iota(jnp.int32, (rank, LANES), 1)
    work = jnp.where(lane < rank, gram[...], jnp.where(lane == row + rank, 1.0, 0.0))
    for j in range(rank - 1):
        pivot = work[j : j + 1, :]
        ratio = jnp.where(row > j, work[:, j : j + 1] / work[j : j + 1, j : j + 1], 0.0)
        work = work - ratio * pivot
    scale = jnp.sum(jnp.where(lane == row, work, 0.0), axis=1, keepdims=True)
    out[...] = work[:, rank : 2 * rank] / jnp.sqrt(scale)


def inverse_factor(gram):
    rank = gram.shape[0]
    return small_call(inverse_kernel, jax.ShapeDtypeStruct((rank, rank), F32), (gram,))


def local(activations, out_grads, error, q_start):
    acts, grads = activations[0], out_grads[0]
    _, width = acts.shape
    own_rows = error.shape[1]
    rank = q_start.shape[1]
    groups = lax.axis_size(GRP)
    side, half = width // 4, width // 8
    chunks = width // LANES
    x, core, y = lax.axis_index("x"), lax.axis_index("c"), lax.axis_index("y")
    core_ref = core.astype(jnp.int32).reshape(1)

    a_own = spread(acts, "z", 1, side)
    g_own = spread(grads, "y", 1, side)
    a_all = ring_gather(a_own, "y")
    g_all = ring_gather(g_own, "z")

    err = error.reshape(own_rows * chunks, LANES)
    mine, other = split_error(err, core_ref, chunks, side)
    other = shift(other, "c", 1).reshape(4 * own_rows, half)
    parts = fold(x, mine.reshape(4 * own_rows, half), other, F32)
    mean = swapped((parts[0] + parts[1]) + (parts[2] + parts[3]))

    seen = [(m, k) for m in (0, 1, 3) for k in (0, 1, 3)]
    rest = [(2, 0), (0, 2), (2, 2), (2, 1), (1, 2), (2, 3), (3, 2)]
    whole = jax.ShapeDtypeStruct((side, side), F32)
    part = jax.ShapeDtypeStruct((side, half), F32)
    smem = pl.BlockSpec(memory_space=pltpu.SMEM)
    block = pl.BlockSpec((HEIGHT, side), lambda i: (i, 0))
    near = block_call(near_kernel, seen, a_all, g_all, [], [], whole)
    rounded, mine, other = block_call(
        rest_kernel, rest, a_all, g_all, [core_ref, near], [smem, block],
        (jax.ShapeDtypeStruct((side, side), BF), part, part),
    )
    parts = fold(x, mine, shift(other, "c", 1), BF)
    pieces = [lax.dynamic_slice_in_dim(rounded, lax.rem(y + k, 4) * own_rows, own_rows, 0) for k in range(4)]
    pieces[1], pieces[3] = shift(pieces[1], "y", 1), shift(pieces[3], "y", 3)
    mean = ((mean + parts[0]) + (parts[1].astype(F32) + parts[2].astype(F32)) + parts[3].astype(F32)) / groups

    right = lax.dynamic_slice_in_dim(q_start[0], y * side + core * half, half, 1)
    left_shape = jax.ShapeDtypeStruct((rank, own_rows), F32)
    right_shape = jax.ShapeDtypeStruct((rank, half + LANES), F32)
    gram_shape = jax.ShapeDtypeStruct((rank, LANES), F32)
    partial = small_call(left_kernel, left_shape, (right, mean))
    for step in range(ITERS):
        partial = partial + shift(partial, "c", 1)
        if step == 0:
            partial, pieces[1], pieces[3] = lax.optimization_barrier((partial, pieces[1], pieces[3]))
            terms = (*ring(partial, "y"), mean)
        else:
            partial, pieces[2] = lax.optimization_barrier((partial, pieces[2]))
            terms = (inverse_factor(gram), *ring(partial, "y"), mean)
        left, both = small_call(functools.partial(right_kernel, step > 0), (left_shape, right_shape), terms)
        if step == 0:
            pieces[2] = shift(after(pieces[2], both), "y", 2)
        own, far, below, above = ring(both, "z")
        both = (own + far) + (below + above)
        if step + 1 < ITERS:
            partial, gram = small_call(left_sum_kernel, (left_shape, gram_shape), (*ring(both, "x"), mean))
    own, far, below, above = ring(both, "x")
    both = (own + far) + (below + above)
    right, gram = both[:, :half], both[:, half:]
    inv = inverse_factor(gram)
    got = jnp.concatenate([right] + [shift(right, "y", k) for k in (1, 2, 3)], axis=0)
    place = jnp.stack([y, core]).astype(jnp.int32)
    right, stacked = small_call(
        factor_kernel,
        (jax.ShapeDtypeStruct((rank, width), F32), jax.ShapeDtypeStruct((3 * rank, width), BF)),
        (inv, got, shift(got, "c", 1)),
        (place,),
    )
    basis = times(inv, swapped(left), ((1,), (0,)))
    update, error_next = finish(basis, stacked, err, pieces)
    return (
        update.reshape(own_rows, 1, width),
        error_next.reshape(1, own_rows, 1, width),
        right[None],
    )


def solution(mesh):
    split = Mesh(mesh.devices.reshape(4, 2, 4, 4), ALL)

    return jax.shard_map(
        local,
        mesh=split,
        in_specs=(
            P(None, ALL, None),
            P(None, ALL, None),
            P(GRP, SHARD, None, None),
            P(),
        ),
        out_specs=(P(SHARD, None, None), P(GRP, SHARD, None, None), P()),
        check_vma=False,
    )
```

```python
import functools

import jax
import jax.numpy as jnp
from jax import lax
from jax.experimental import pallas as pl
from jax.experimental.pallas import tpu as pltpu
from jax.sharding import Mesh
from jax.sharding import PartitionSpec as P

GRP = ("x", "c")
SHARD = ("z", "y")
ALL = ("x", "c", "z", "y")
BF = jnp.bfloat16
F32 = jnp.float32
HIGH = lax.Precision.HIGHEST
ITERS = 2
LANES = 128
HEIGHT = 256
FULL = 60 * 2**20


def shift(v, axis, by):
    n = lax.axis_size(axis)
    return lax.ppermute(v, axis, [(i, (i + by) % n) for i in range(n)])


def swapped(v):
    n = lax.axis_size("x")
    pairs = [(i * n + j, j * n + i) for i in range(n) for j in range(n)]
    return lax.ppermute(v, ("x", "y"), pairs)


def times(a, b, dims):
    return lax.dot_general(a, b, (dims, ((), ())), precision=HIGH)


def spread(v, axis, dim, size):
    n = lax.axis_size(axis)
    me = lax.axis_index(axis)
    got = []
    for k in range(n):
        piece = lax.dynamic_slice_in_dim(v, lax.rem(me + k, n) * size, size, dim)
        if k > 0:
            piece = shift(piece, axis, k)
        got.append(piece)
    return got


def ring_gather(pieces, axis):
    below = [shift(v, axis, 1) for v in pieces]
    above = [shift(v, axis, -1) for v in pieces]
    far = []
    for k in range(4):
        far.append(shift((below if k < 2 else above)[k], axis, 1 if k < 2 else -1))
    return [pieces, below, far, above]


def split_kernel(core, err, mine, other):
    rows, chunks = mine.shape[1], err.shape[0] // mine.shape[1]
    per = mine.shape[2] // LANES
    for b in range(mine.shape[0]):
        for j in range(per):
            lanes = slice(j * LANES, (j + 1) * LANES)
            for out, half in ((mine, core[0]), (other, 1 - core[0])):
                out[b, :, lanes] = err[pl.ds(2 * per * b + per * half + j, rows, stride=chunks), :]


def split_error(err, core, chunks, side):
    rows = err.shape[0] // chunks
    step = 64
    shape = jax.ShapeDtypeStruct((4, rows, side // 2), F32)
    out = pl.BlockSpec((4, step, side // 2), lambda i, s: (0, i, 0))
    return pl.pallas_call(
        split_kernel,
        out_shape=(shape, shape),
        grid_spec=pltpu.PrefetchScalarGridSpec(
            num_scalar_prefetch=1,
            grid=(rows // step,),
            in_specs=[pl.BlockSpec((step * chunks, LANES), lambda i, s: (i, 0))],
            out_specs=(out, out),
        ),
        compiler_params=pltpu.CompilerParams(vmem_limit_bytes=FULL),
        cost_estimate=pl.CostEstimate(flops=10**6, bytes_accessed=8 * err.size, transcendentals=0),
    )(core, err)


def fold_kernel(x, mine, theirs, own, *sent):
    k = pl.program_id(0)
    total = mine[...] + theirs[...]

    @pl.when(k == 0)
    def _():
        own[...] = total

    for j, out in enumerate(sent):

        @pl.when(k == j + 1)
        def _(out=out):
            out[...] = total.astype(out.dtype)


def fold(x, mine, theirs, dtype):
    rows, width = mine.shape[0] // 4, mine.shape[1]
    taken = pl.BlockSpec((rows, width), lambda k, s: (lax.rem(s[0] + k, 4), 0))
    fixed = pl.BlockSpec((rows, width), lambda k, s: (0, 0))
    sent = jax.ShapeDtypeStruct((rows, width), dtype)
    parts = pl.pallas_call(
        fold_kernel,
        out_shape=(jax.ShapeDtypeStruct((rows, width), F32), sent, sent, sent),
        grid_spec=pltpu.PrefetchScalarGridSpec(
            num_scalar_prefetch=1, grid=(4,), in_specs=[taken, taken], out_specs=(fixed,) * 4
        ),
        compiler_params=pltpu.CompilerParams(vmem_limit_bytes=FULL),
        cost_estimate=pl.CostEstimate(flops=10**6, bytes_accessed=40 * rows * width, transcendentals=0),
    )(x.astype(jnp.int32).reshape(1), mine, theirs)
    return [parts[0]] + [shift(parts[k], "x", k) for k in (1, 2, 3)]


def pair_copies(n, refs, sa, sg, sems):
    toks = sa.shape[0] // n
    copies = []
    for i in range(n):
        rows = pl.ds(i * toks, toks)
        left = pltpu.make_async_copy(refs[i], sa.at[rows], sems.at[i])
        right = pltpu.make_async_copy(refs[n + i], sg.at[rows], sems.at[n + i])
        copies.append((left, right))
    return copies


def product(sa, sg, rows, lanes):
    dims = (((0,), (0,)), ((), ()))
    return lax.dot_general(sa[rows, lanes], sg[rows, :], dims, preferred_element_type=F32)


def block_rows(n, refs, sa, sg, sems, height, store):
    step = pl.program_id(0)
    toks = sa.shape[0] // n

    @pl.when(step == 0)
    def _():
        copies = pair_copies(n, refs, sa, sg, sems)
        for left, right in copies:
            left.start()
            right.start()
        total = None
        for low in range(0, n, 3):
            high = min(low + 3, n)
            for left, right in copies[low:high]:
                left.wait()
                right.wait()
            part = product(sa, sg, slice(low * toks, high * toks), slice(0, height))
            total = part if total is None else total + part
        store(total)

    @pl.when(step > 0)
    def _():
        lanes = pl.ds(pl.multiple_of(step * height, height), height)
        store(product(sa, sg, slice(0, n * toks), lanes))


def near_kernel(n, *refs):
    out, sa, sg, sems = refs[-4:]
    height = out.shape[0]

    @pl.when(pl.program_id(0) == 0)
    def _():
        copies = pair_copies(n, refs, sa, sg, sems)
        for left, right in copies:
            left.start()
            right.start()
        for left, right in copies:
            left.wait()
            right.wait()

    lanes = pl.ds(pl.multiple_of(pl.program_id(0) * height, height), height)
    out[...] = product(sa, sg, slice(0, sa.shape[0]), lanes)


def rest_kernel(n, *refs):
    core, start, right, rounded, mine, other, left, sa, sg, sems = refs[-10:]
    half = mine.shape[1]

    def store(total):
        total = start[...] + total
        rounded[...] = total.astype(BF)
        first = core[0] == 0
        low, high = total[:, :half], total[:, half:]
        mine[...] = jnp.where(first, low, high)
        other[...] = jnp.where(first, high, low)

    block_rows(n, refs, sa, sg, sems, start.shape[0], store)
    first = core[0] == 0
    low, high = right[:, :half], right[:, half:]
    total = dot(jnp.where(first, low, high), mine[...], ((1,), (1,)))
    left[...] = total + dot(jnp.where(first, high, low), other[...], ((1,), (1,)))


def block_spec(v):
    if v.shape[0] < HEIGHT:
        return pl.BlockSpec((v.shape[0], HEIGHT), lambda i: (0, i))
    return pl.BlockSpec((HEIGHT, v.shape[1]), lambda i: (i, 0))


def block_call(kernel, pairs, a_all, g_all, extra, extra_specs, shapes):
    a = [a_all[m][k] for m, k in pairs]
    g = [g_all[k][m] for m, k in pairs]
    n, (toks, side) = len(pairs), a[0].shape
    moved = 4 * n * toks * side + 4 * side * side
    return pl.pallas_call(
        functools.partial(kernel, n),
        grid=(side // HEIGHT,),
        out_shape=shapes,
        in_specs=[pl.BlockSpec(memory_space=pl.ANY)] * (2 * n) + extra_specs,
        out_specs=jax.tree.map(block_spec, shapes),
        scratch_shapes=[
            pltpu.VMEM((n * toks, side), BF),
            pltpu.VMEM((n * toks, side), BF),
            pltpu.SemaphoreType.DMA((2 * n,)),
        ],
        compiler_params=pltpu.CompilerParams(vmem_limit_bytes=FULL),
        cost_estimate=pl.CostEstimate(flops=2 * n * toks * side * side, bytes_accessed=moved, transcendentals=0),
    )(*a, *g, *extra)


def small_call(kernel, shapes, args, scalars=()):
    spec = pl.BlockSpec(memory_space=pltpu.VMEM)
    return pl.pallas_call(
        kernel,
        out_shape=shapes,
        in_specs=[pl.BlockSpec(memory_space=pltpu.SMEM)] * len(scalars) + [spec] * len(args),
        out_specs=jax.tree.map(lambda _: spec, shapes),
        compiler_params=pltpu.CompilerParams(vmem_limit_bytes=16 * 2**20),
        cost_estimate=pl.CostEstimate(flops=2 * 10**8, bytes_accessed=10**6, transcendentals=0),
    )(*scalars, *args)


def dot(a, b, dims):
    return lax.dot_general(a, b, (dims, ((), ())), precision=HIGH, preferred_element_type=F32)


def left_kernel(right, mean, out):
    out[...] = dot(right[...], mean[...], ((1,), (1,)))


def left_sum_kernel(own, far, below, above, mean, out, gram):
    half = mean.shape[1]
    right = (own[...] + far[...]) + (below[...] + above[...])
    out[...] = dot(right[:, :half], mean[...], ((1,), (1,)))
    gram[...] = right[:, half : half + LANES]


def right_kernel(scaled, *refs):
    if scaled:
        inv, own, far, below, above, mean, left_out, out = refs
    else:
        own, far, below, above, mean, left_out, out = refs
    left = (own[...] + far[...]) + (below[...] + above[...])
    if scaled:
        left = dot(inv[...], left, ((1,), (0,)))
    half = mean.shape[1]
    left_out[...] = left
    out[:, :half] = dot(left, mean[...], ((1,), (0,)))
    out[:, half:] = jnp.zeros((left.shape[0], LANES), F32)
    out[:, half : half + left.shape[0]] = dot(left, left, ((1,), (1,)))


def factor_kernel(place, inv, mine, theirs, factor, stacked):
    rank = inv.shape[0]
    half = mine.shape[1]
    y, core = place[0], place[1]
    for b in range(4):
        k = lax.rem(y - b + 4, 4)
        rows = pl.ds(pl.multiple_of(k * rank, rank), rank)
        ours, others = mine[rows, :], theirs[rows, :]
        for h in range(2):
            lanes = slice((2 * b + h) * half, (2 * b + h + 1) * half)
            value = dot(inv[...], jnp.where(core == h, ours, others), ((1,), (0,)))
            factor[:, lanes] = value
            hi = value.astype(BF)
            lo = (value - hi.astype(F32)).astype(BF)
            stacked[0:rank, lanes] = hi
            stacked[rank : 2 * rank, lanes] = lo
            stacked[2 * rank : 3 * rank, lanes] = hi


def ring(v, axis):
    return v, shift(v, axis, 2), shift(v, axis, 1), shift(v, axis, -1)


def final_kernel(me, basis, factor, err, g0, g1, g2, g3, update, error_next):
    rows, chunks = basis.shape[0], factor.shape[1] // LANES
    per = g0.shape[1] // LANES
    for j in range(chunks):
        at, lanes = pl.ds(j, rows, stride=chunks), slice(j * LANES, (j + 1) * LANES)
        b, own = j // per, slice((j % per) * LANES, (j % per + 1) * LANES)
        k = lax.rem(me[0] - b + 4, 4)
        new = jnp.dot(basis[...], factor[:, lanes], preferred_element_type=F32)
        grad = jnp.where(
            k < 2,
            jnp.where(k == 0, g0[:, own].astype(F32), g1[:, own].astype(F32)),
            jnp.where(k == 2, g2[:, own].astype(F32), g3[:, own].astype(F32)),
        )
        update[at, :] = new
        error_next[at, :] = grad + err[at, :] - new


def basis_terms(basis):
    b = basis.T
    hi = lax.reduce_precision(b, 8, 7)
    return jnp.concatenate([hi, hi, b - hi], axis=1).astype(BF)


def finish(basis, right3, err, pieces):
    left3 = basis_terms(basis)
    own_rows, width = basis.shape[1], right3.shape[1]
    side = pieces[0].shape[1]
    step = 64
    chunks = width // LANES
    me = lax.axis_index("y").astype(jnp.int32).reshape(1)
    tall = pl.BlockSpec((step * chunks, LANES), lambda i, s: (i, 0))
    grads = pl.BlockSpec((step, side), lambda i, s: (i, 0))
    shape = jax.ShapeDtypeStruct((own_rows * chunks, LANES), F32)
    return pl.pallas_call(
        final_kernel,
        out_shape=(shape, shape),
        grid_spec=pltpu.PrefetchScalarGridSpec(
            num_scalar_prefetch=1,
            grid=(own_rows // step,),
            in_specs=[
                pl.BlockSpec((step, left3.shape[1]), lambda i, s: (i, 0)),
                pl.BlockSpec(right3.shape, lambda i, s: (0, 0)),
                tall,
                *[grads] * 4,
            ],
            out_specs=(tall, tall),
        ),
        compiler_params=pltpu.CompilerParams(vmem_limit_bytes=40 * 2**20),
        cost_estimate=pl.CostEstimate(flops=2 * 96 * own_rows * width, bytes_accessed=14 * own_rows * width, transcendentals=0),
    )(me, left3, right3, err, *pieces)


def inverse_kernel(gram, out):
    rank = gram.shape[0]
    row = lax.broadcasted_iota(jnp.int32, (rank, LANES), 0)
    lane = lax.broadcasted_iota(jnp.int32, (rank, LANES), 1)
    work = jnp.where(lane < rank, gram[...], jnp.where(lane == row + rank, 1.0, 0.0))
    for j in range(rank - 1):
        pivot = work[j : j + 1, :]
        ratio = jnp.where(row > j, work[:, j : j + 1] / work[j : j + 1, j : j + 1], 0.0)
        work = work - ratio * pivot
    scale = jnp.sum(jnp.where(lane == row, work, 0.0), axis=1, keepdims=True)
    out[...] = work[:, rank : 2 * rank] / jnp.sqrt(scale)


def inverse_factor(gram):
    rank = gram.shape[0]
    return small_call(inverse_kernel, jax.ShapeDtypeStruct((rank, rank), F32), (gram,))


def local(activations, out_grads, error, q_start):
    acts, grads = activations[0], out_grads[0]
    _, width = acts.shape
    own_rows = error.shape[1]
    rank = q_start.shape[1]
    groups = lax.axis_size(GRP)
    side, half = width // 4, width // 8
    chunks = width // LANES
    x, core, y = lax.axis_index("x"), lax.axis_index("c"), lax.axis_index("y")
    core_ref = core.astype(jnp.int32).reshape(1)

    a_own = spread(acts, "z", 1, side)
    g_own = spread(grads, "y", 1, side)
    a_all = ring_gather(a_own, "y")
    g_all = ring_gather(g_own, "z")

    err = error.reshape(own_rows * chunks, LANES)
    mine, other = split_error(err, core_ref, chunks, side)
    other = shift(other, "c", 1).reshape(4 * own_rows, half)
    parts = fold(x, mine.reshape(4 * own_rows, half), other, F32)
    mean = swapped((parts[0] + parts[1]) + (parts[2] + parts[3]))

    seen = [(m, k) for m in (0, 1, 3) for k in (0, 1, 3)]
    rest = [(2, 0), (0, 2), (2, 2), (2, 1), (1, 2), (2, 3), (3, 2)]
    whole = jax.ShapeDtypeStruct((side, side), F32)
    part = jax.ShapeDtypeStruct((side, half), F32)
    smem = pl.BlockSpec(memory_space=pltpu.SMEM)
    block = pl.BlockSpec((HEIGHT, side), lambda i: (i, 0))
    near = block_call(near_kernel, seen, a_all, g_all, [], [], whole)
    right = lax.dynamic_slice_in_dim(q_start[0], y * side, side, 1)
    start_spec = pl.BlockSpec(right.shape, lambda i: (0, 0))
    rounded, mine, other, partial = block_call(
        rest_kernel, rest, a_all, g_all, [core_ref, near, right], [smem, block, start_spec],
        (jax.ShapeDtypeStruct((side, side), BF), part, part, jax.ShapeDtypeStruct(right.shape, F32)),
    )
    theirs = shift(other, "c", 1)
    terms = spread(partial, "x", 1, own_rows)
    right = lax.dynamic_slice_in_dim(right, core * half, half, 1)
    partial = small_call(left_kernel, jax.ShapeDtypeStruct((rank, own_rows), F32), (right, mean))
    partial = (partial + (terms[0] + terms[2])) + (terms[1] + terms[3])
    partial = (partial + shift(partial, "c", 1)) / groups
    first = (partial, shift(partial, "y", 2), shift(partial, "y", 1), shift(partial, "y", -1))
    parts = fold(x, mine, theirs, BF)
    pieces = [lax.dynamic_slice_in_dim(rounded, lax.rem(y + k, 4) * own_rows, own_rows, 0) for k in range(4)]
    pieces = pieces[:1] + [shift(pieces[k], "y", k) for k in (1, 2, 3)]
    mean = ((mean + parts[0]) + (parts[1].astype(F32) + parts[2].astype(F32)) + parts[3].astype(F32)) / groups

    left_shape = jax.ShapeDtypeStruct((rank, own_rows), F32)
    right_shape = jax.ShapeDtypeStruct((rank, half + LANES), F32)
    gram_shape = jax.ShapeDtypeStruct((rank, LANES), F32)
    for step in range(ITERS):
        if step == 0:
            terms = (*first, mean)
        else:
            partial = partial + shift(partial, "c", 1)
            partial, pieces = lax.optimization_barrier((partial, pieces))
            terms = (inverse_factor(gram), *ring(partial, "y"), mean)
        left, both = small_call(functools.partial(right_kernel, step > 0), (left_shape, right_shape), terms)
        own, far, below, above = ring(both, "z")
        both = (own + far) + (below + above)
        if step + 1 < ITERS:
            partial, gram = small_call(left_sum_kernel, (left_shape, gram_shape), (*ring(both, "x"), mean))
    own, far, below, above = ring(both, "x")
    both = (own + far) + (below + above)
    right, gram = both[:, :half], both[:, half:]
    inv = inverse_factor(gram)
    got = jnp.concatenate([right] + [shift(right, "y", k) for k in (1, 2, 3)], axis=0)
    place = jnp.stack([y, core]).astype(jnp.int32)
    right, stacked = small_call(
        factor_kernel,
        (jax.ShapeDtypeStruct((rank, width), F32), jax.ShapeDtypeStruct((3 * rank, width), BF)),
        (inv, got, shift(got, "c", 1)),
        (place,),
    )
    basis = times(inv, swapped(left), ((1,), (0,)))
    update, error_next = finish(basis, stacked, err, pieces)
    return (
        update.reshape(own_rows, 1, width),
        error_next.reshape(1, own_rows, 1, width),
        right[None],
    )


def solution(mesh):
    split = Mesh(mesh.devices.reshape(4, 2, 4, 4), ALL)

    return jax.shard_map(
        local,
        mesh=split,
        in_specs=(
            P(None, ALL, None),
            P(None, ALL, None),
            P(GRP, SHARD, None, None),
            P(),
        ),
        out_specs=(P(SHARD, None, None), P(GRP, SHARD, None, None), P()),
        check_vma=False,
    )
```

```python
import functools

import jax
import jax.numpy as jnp
from jax import lax
from jax.experimental import pallas as pl
from jax.experimental.pallas import tpu as pltpu
from jax.sharding import Mesh
from jax.sharding import PartitionSpec as P

GRP = ("x", "c")
SHARD = ("z", "y")
ALL = ("x", "c", "z", "y")
BF = jnp.bfloat16
F32 = jnp.float32
HIGH = lax.Precision.HIGHEST
ITERS = 2
LANES = 128
HEIGHT = 256
FULL = 60 * 2**20


def shift(v, axis, by):
    n = lax.axis_size(axis)
    return lax.ppermute(v, axis, [(i, (i + by) % n) for i in range(n)])


def swapped(v):
    n = lax.axis_size("x")
    pairs = [(i * n + j, j * n + i) for i in range(n) for j in range(n)]
    return lax.ppermute(v, ("x", "y"), pairs)


def times(a, b, dims):
    return lax.dot_general(a, b, (dims, ((), ())), precision=HIGH)


def spread(v, axis, dim, size):
    n = lax.axis_size(axis)
    me = lax.axis_index(axis)
    got = []
    for k in range(n):
        piece = lax.dynamic_slice_in_dim(v, lax.rem(me + k, n) * size, size, dim)
        if k > 0:
            piece = shift(piece, axis, k)
        got.append(piece)
    return got


def ring_gather(pieces, axis):
    below = [shift(v, axis, 1) for v in pieces]
    above = [shift(v, axis, -1) for v in pieces]
    far = []
    for k in range(4):
        far.append(shift((below if k < 2 else above)[k], axis, 1 if k < 2 else -1))
    return [pieces, below, far, above]


def split_kernel(core, err, mine, other):
    rows, chunks = mine.shape[1], err.shape[0] // mine.shape[1]
    per = mine.shape[2] // LANES
    for b in range(mine.shape[0]):
        for j in range(per):
            lanes = slice(j * LANES, (j + 1) * LANES)
            for out, half in ((mine, core[0]), (other, 1 - core[0])):
                out[b, :, lanes] = err[pl.ds(2 * per * b + per * half + j, rows, stride=chunks), :]


def split_error(err, core, chunks, side):
    rows = err.shape[0] // chunks
    step = 64
    shape = jax.ShapeDtypeStruct((4, rows, side // 2), F32)
    out = pl.BlockSpec((4, step, side // 2), lambda i, s: (0, i, 0))
    return pl.pallas_call(
        split_kernel,
        out_shape=(shape, shape),
        grid_spec=pltpu.PrefetchScalarGridSpec(
            num_scalar_prefetch=1,
            grid=(rows // step,),
            in_specs=[pl.BlockSpec((step * chunks, LANES), lambda i, s: (i, 0))],
            out_specs=(out, out),
        ),
        compiler_params=pltpu.CompilerParams(vmem_limit_bytes=FULL),
        cost_estimate=pl.CostEstimate(flops=10**6, bytes_accessed=8 * err.size, transcendentals=0),
    )(core, err)


def fold_kernel(x, mine, theirs, own, *sent):
    k = pl.program_id(0)
    total = mine[...] + theirs[...]

    @pl.when(k == 0)
    def _():
        own[...] = total

    for j, out in enumerate(sent):

        @pl.when(k == j + 1)
        def _(out=out):
            out[...] = total.astype(out.dtype)


def fold(x, mine, theirs, dtype):
    rows, width = mine.shape[0] // 4, mine.shape[1]
    taken = pl.BlockSpec((rows, width), lambda k, s: (lax.rem(s[0] + k, 4), 0))
    fixed = pl.BlockSpec((rows, width), lambda k, s: (0, 0))
    sent = jax.ShapeDtypeStruct((rows, width), dtype)
    parts = pl.pallas_call(
        fold_kernel,
        out_shape=(jax.ShapeDtypeStruct((rows, width), F32), sent, sent, sent),
        grid_spec=pltpu.PrefetchScalarGridSpec(
            num_scalar_prefetch=1, grid=(4,), in_specs=[taken, taken], out_specs=(fixed,) * 4
        ),
        compiler_params=pltpu.CompilerParams(vmem_limit_bytes=FULL),
        cost_estimate=pl.CostEstimate(flops=10**6, bytes_accessed=40 * rows * width, transcendentals=0),
    )(x.astype(jnp.int32).reshape(1), mine, theirs)
    return [parts[0]] + [shift(parts[k], "x", k) for k in (1, 2, 3)]


def pair_copies(n, refs, sa, sg, sems):
    toks = sa.shape[0] // n
    copies = []
    for i in range(n):
        rows = pl.ds(i * toks, toks)
        left = pltpu.make_async_copy(refs[i], sa.at[rows], sems.at[i])
        right = pltpu.make_async_copy(refs[n + i], sg.at[rows], sems.at[n + i])
        copies.append((left, right))
    return copies


def product(sa, sg, rows, lanes):
    dims = (((0,), (0,)), ((), ()))
    return lax.dot_general(sa[rows, lanes], sg[rows, :], dims, preferred_element_type=F32)


def block_rows(n, refs, sa, sg, sems, height, store):
    step = pl.program_id(0)
    toks = sa.shape[0] // n

    @pl.when(step == 0)
    def _():
        copies = pair_copies(n, refs, sa, sg, sems)
        for left, right in copies:
            left.start()
            right.start()
        total = None
        for low in range(0, n, 3):
            high = min(low + 3, n)
            for left, right in copies[low:high]:
                left.wait()
                right.wait()
            part = product(sa, sg, slice(low * toks, high * toks), slice(0, height))
            total = part if total is None else total + part
        store(total)

    @pl.when(step > 0)
    def _():
        lanes = pl.ds(pl.multiple_of(step * height, height), height)
        store(product(sa, sg, slice(0, n * toks), lanes))


def near_kernel(n, *refs):
    out, sa, sg, sems = refs[-4:]
    height = out.shape[0]

    @pl.when(pl.program_id(0) == 0)
    def _():
        copies = pair_copies(n, refs, sa, sg, sems)
        for left, right in copies:
            left.start()
            right.start()
        for left, right in copies:
            left.wait()
            right.wait()

    lanes = pl.ds(pl.multiple_of(pl.program_id(0) * height, height), height)
    out[...] = product(sa, sg, slice(0, sa.shape[0]), lanes)


def rest_kernel(n, *refs):
    core, start, right, rounded, mine, other, left, sa, sg, sems = refs[-10:]
    half = mine.shape[1]

    def store(total):
        total = start[...] + total
        rounded[...] = total.astype(BF)
        first = core[0] == 0
        low, high = total[:, :half], total[:, half:]
        mine[...] = jnp.where(first, low, high)
        other[...] = jnp.where(first, high, low)

    block_rows(n, refs, sa, sg, sems, start.shape[0], store)
    dims = (((1,), (1,)), ((), ()))
    both = lax.dot_general(right[...], rounded[...], dims, preferred_element_type=F32)
    rank = left.shape[0]
    left[...] = both[:rank] + both[rank:]


def block_spec(v):
    if v.shape[0] < HEIGHT:
        return pl.BlockSpec((v.shape[0], HEIGHT), lambda i: (0, i))
    return pl.BlockSpec((HEIGHT, v.shape[1]), lambda i: (i, 0))


def block_call(kernel, pairs, a_all, g_all, extra, extra_specs, shapes):
    a = [a_all[m][k] for m, k in pairs]
    g = [g_all[k][m] for m, k in pairs]
    n, (toks, side) = len(pairs), a[0].shape
    moved = 4 * n * toks * side + 4 * side * side
    return pl.pallas_call(
        functools.partial(kernel, n),
        grid=(side // HEIGHT,),
        out_shape=shapes,
        in_specs=[pl.BlockSpec(memory_space=pl.ANY)] * (2 * n) + extra_specs,
        out_specs=jax.tree.map(block_spec, shapes),
        scratch_shapes=[
            pltpu.VMEM((n * toks, side), BF),
            pltpu.VMEM((n * toks, side), BF),
            pltpu.SemaphoreType.DMA((2 * n,)),
        ],
        compiler_params=pltpu.CompilerParams(vmem_limit_bytes=FULL),
        cost_estimate=pl.CostEstimate(flops=2 * n * toks * side * side, bytes_accessed=moved, transcendentals=0),
    )(*a, *g, *extra)


def small_call(kernel, shapes, args, scalars=()):
    spec = pl.BlockSpec(memory_space=pltpu.VMEM)
    return pl.pallas_call(
        kernel,
        out_shape=shapes,
        in_specs=[pl.BlockSpec(memory_space=pltpu.SMEM)] * len(scalars) + [spec] * len(args),
        out_specs=jax.tree.map(lambda _: spec, shapes),
        compiler_params=pltpu.CompilerParams(vmem_limit_bytes=16 * 2**20),
        cost_estimate=pl.CostEstimate(flops=2 * 10**8, bytes_accessed=10**6, transcendentals=0),
    )(*scalars, *args)


def dot(a, b, dims):
    return lax.dot_general(a, b, (dims, ((), ())), precision=HIGH, preferred_element_type=F32)


def left_kernel(right, mean, out):
    out[...] = dot(right[...], mean[...], ((1,), (1,)))


def left_sum_kernel(own, far, below, above, mean, out, gram):
    half = mean.shape[1]
    right = (own[...] + far[...]) + (below[...] + above[...])
    out[...] = dot(right[:, :half], mean[...], ((1,), (1,)))
    gram[...] = right[:, half : half + LANES]


def right_kernel(scaled, *refs):
    if scaled:
        inv, own, far, below, above, mean, left_out, out = refs
    else:
        own, far, below, above, mean, left_out, out = refs
    left = (own[...] + far[...]) + (below[...] + above[...])
    if scaled:
        left = dot(inv[...], left, ((1,), (0,)))
    half = mean.shape[1]
    left_out[...] = left
    out[:, :half] = dot(left, mean[...], ((1,), (0,)))
    out[:, half:] = jnp.zeros((left.shape[0], LANES), F32)
    out[:, half : half + left.shape[0]] = dot(left, left, ((1,), (1,)))


def factor_kernel(place, inv, mine, theirs, factor, stacked):
    rank = inv.shape[0]
    half = mine.shape[1]
    y, core = place[0], place[1]
    for b in range(4):
        k = lax.rem(y - b + 4, 4)
        rows = pl.ds(pl.multiple_of(k * rank, rank), rank)
        ours, others = mine[rows, :], theirs[rows, :]
        for h in range(2):
            lanes = slice((2 * b + h) * half, (2 * b + h + 1) * half)
            value = dot(inv[...], jnp.where(core == h, ours, others), ((1,), (0,)))
            factor[:, lanes] = value
            hi = value.astype(BF)
            lo = (value - hi.astype(F32)).astype(BF)
            stacked[0:rank, lanes] = hi
            stacked[rank : 2 * rank, lanes] = lo
            stacked[2 * rank : 3 * rank, lanes] = hi


def ring(v, axis):
    return v, shift(v, axis, 2), shift(v, axis, 1), shift(v, axis, -1)


def after(v, token):
    return lax.optimization_barrier((v, token))[0]


def final_kernel(me, basis, factor, err, g0, g1, g2, g3, update, error_next):
    rows, chunks = basis.shape[0], factor.shape[1] // LANES
    per = g0.shape[1] // LANES
    for j in range(chunks):
        at, lanes = pl.ds(j, rows, stride=chunks), slice(j * LANES, (j + 1) * LANES)
        b, own = j // per, slice((j % per) * LANES, (j % per + 1) * LANES)
        k = lax.rem(me[0] - b + 4, 4)
        new = jnp.dot(basis[...], factor[:, lanes], preferred_element_type=F32)
        grad = jnp.where(
            k < 2,
            jnp.where(k == 0, g0[:, own].astype(F32), g1[:, own].astype(F32)),
            jnp.where(k == 2, g2[:, own].astype(F32), g3[:, own].astype(F32)),
        )
        update[at, :] = new
        error_next[at, :] = grad + err[at, :] - new


def basis_terms(basis):
    b = basis.T
    hi = lax.reduce_precision(b, 8, 7)
    return jnp.concatenate([hi, hi, b - hi], axis=1).astype(BF)


def finish(basis, right3, err, pieces):
    left3 = basis_terms(basis)
    own_rows, width = basis.shape[1], right3.shape[1]
    side = pieces[0].shape[1]
    step = 64
    chunks = width // LANES
    me = lax.axis_index("y").astype(jnp.int32).reshape(1)
    tall = pl.BlockSpec((step * chunks, LANES), lambda i, s: (i, 0))
    grads = pl.BlockSpec((step, side), lambda i, s: (i, 0))
    shape = jax.ShapeDtypeStruct((own_rows * chunks, LANES), F32)
    return pl.pallas_call(
        final_kernel,
        out_shape=(shape, shape),
        grid_spec=pltpu.PrefetchScalarGridSpec(
            num_scalar_prefetch=1,
            grid=(own_rows // step,),
            in_specs=[
                pl.BlockSpec((step, left3.shape[1]), lambda i, s: (i, 0)),
                pl.BlockSpec(right3.shape, lambda i, s: (0, 0)),
                tall,
                *[grads] * 4,
            ],
            out_specs=(tall, tall),
        ),
        compiler_params=pltpu.CompilerParams(vmem_limit_bytes=40 * 2**20),
        cost_estimate=pl.CostEstimate(flops=2 * 96 * own_rows * width, bytes_accessed=14 * own_rows * width, transcendentals=0),
    )(me, left3, right3, err, *pieces)


def inverse_kernel(gram, out):
    rank = gram.shape[0]
    row = lax.broadcasted_iota(jnp.int32, (rank, LANES), 0)
    lane = lax.broadcasted_iota(jnp.int32, (rank, LANES), 1)
    work = jnp.where(lane < rank, gram[...], jnp.where(lane == row + rank, 1.0, 0.0))
    for j in range(rank - 1):
        pivot = work[j : j + 1, :]
        ratio = jnp.where(row > j, work[:, j : j + 1] / work[j : j + 1, j : j + 1], 0.0)
        work = work - ratio * pivot
    scale = jnp.sum(jnp.where(lane == row, work, 0.0), axis=1, keepdims=True)
    out[...] = work[:, rank : 2 * rank] / jnp.sqrt(scale)


def inverse_factor(gram):
    rank = gram.shape[0]
    return small_call(inverse_kernel, jax.ShapeDtypeStruct((rank, rank), F32), (gram,))


def local(activations, out_grads, error, q_start):
    acts, grads = activations[0], out_grads[0]
    _, width = acts.shape
    own_rows = error.shape[1]
    rank = q_start.shape[1]
    groups = lax.axis_size(GRP)
    side, half = width // 4, width // 8
    chunks = width // LANES
    x, core, y = lax.axis_index("x"), lax.axis_index("c"), lax.axis_index("y")
    core_ref = core.astype(jnp.int32).reshape(1)

    a_own = spread(acts, "z", 1, side)
    g_own = spread(grads, "y", 1, side)
    a_all = ring_gather(a_own, "y")
    g_all = ring_gather(g_own, "z")

    err = error.reshape(own_rows * chunks, LANES)
    mine, other = split_error(err, core_ref, chunks, side)
    other = shift(other, "c", 1).reshape(4 * own_rows, half)
    parts = fold(x, mine.reshape(4 * own_rows, half), other, F32)
    mean = swapped((parts[0] + parts[1]) + (parts[2] + parts[3]))

    seen = [(m, k) for m in (0, 1, 3) for k in (0, 1, 3)]
    rest = [(2, 0), (0, 2), (2, 2), (2, 1), (1, 2), (2, 3), (3, 2)]
    whole = jax.ShapeDtypeStruct((side, side), F32)
    part = jax.ShapeDtypeStruct((side, half), F32)
    smem = pl.BlockSpec(memory_space=pltpu.SMEM)
    block = pl.BlockSpec((HEIGHT, side), lambda i: (i, 0))
    near = block_call(near_kernel, seen, a_all, g_all, [], [], whole)
    right = lax.dynamic_slice_in_dim(q_start[0], y * side, side, 1)
    right_hi = lax.reduce_precision(right, 8, 7)
    two = jnp.concatenate([right_hi, right - right_hi], axis=0).astype(BF)
    start_spec = pl.BlockSpec(two.shape, lambda i: (0, 0))
    rounded, mine, other, partial = block_call(
        rest_kernel, rest, a_all, g_all, [core_ref, near, two], [smem, block, start_spec],
        (jax.ShapeDtypeStruct((side, side), BF), part, part, jax.ShapeDtypeStruct(right.shape, F32)),
    )
    theirs = shift(other, "c", 1)
    terms = spread(partial, "x", 1, own_rows)
    parts = fold(x, mine, theirs, BF)
    terms, right = after((terms, right), parts[0])
    right = lax.dynamic_slice_in_dim(right, core * half, half, 1)
    partial = small_call(left_kernel, jax.ShapeDtypeStruct((rank, own_rows), F32), (right, mean))
    partial = (partial + (terms[0] + terms[2])) + (terms[1] + terms[3])
    partial = (partial + shift(partial, "c", 1)) / groups
    first = (partial, shift(partial, "y", 2), shift(partial, "y", 1), shift(partial, "y", -1))
    pieces = [lax.dynamic_slice_in_dim(rounded, lax.rem(y + k, 4) * own_rows, own_rows, 0) for k in range(4)]
    pieces = pieces[:1] + [shift(pieces[k], "y", k) for k in (1, 2, 3)]
    mean = ((mean + parts[0]) + (parts[1].astype(F32) + parts[2].astype(F32)) + parts[3].astype(F32)) / groups

    left_shape = jax.ShapeDtypeStruct((rank, own_rows), F32)
    right_shape = jax.ShapeDtypeStruct((rank, half + LANES), F32)
    gram_shape = jax.ShapeDtypeStruct((rank, LANES), F32)
    for step in range(ITERS):
        if step == 0:
            terms = (*first, mean)
        else:
            partial = partial + shift(partial, "c", 1)
            terms = (inverse_factor(gram), *ring(partial, "y"), mean)
        left, both = small_call(functools.partial(right_kernel, step > 0), (left_shape, right_shape), terms)
        own, far, below, above = ring(both, "z")
        both = (own + far) + (below + above)
        if step + 1 < ITERS:
            partial, gram = small_call(left_sum_kernel, (left_shape, gram_shape), (*ring(both, "x"), mean))
    own, far, below, above = ring(both, "x")
    both = (own + far) + (below + above)
    right, gram = both[:, :half], both[:, half:]
    inv = inverse_factor(gram)
    got = jnp.concatenate([right] + [shift(right, "y", k) for k in (1, 2, 3)], axis=0)
    place = jnp.stack([y, core]).astype(jnp.int32)
    right, stacked = small_call(
        factor_kernel,
        (jax.ShapeDtypeStruct((rank, width), F32), jax.ShapeDtypeStruct((3 * rank, width), BF)),
        (inv, got, shift(got, "c", 1)),
        (place,),
    )
    basis = times(inv, swapped(left), ((1,), (0,)))
    update, error_next = finish(basis, stacked, err, pieces)
    return (
        update.reshape(own_rows, 1, width),
        error_next.reshape(1, own_rows, 1, width),
        right[None],
    )


def solution(mesh):
    split = Mesh(mesh.devices.reshape(4, 2, 4, 4), ALL)

    return jax.shard_map(
        local,
        mesh=split,
        in_specs=(
            P(None, ALL, None),
            P(None, ALL, None),
            P(GRP, SHARD, None, None),
            P(),
        ),
        out_specs=(P(SHARD, None, None), P(GRP, SHARD, None, None), P()),
        check_vma=False,
    )
```
